32 devices in a mesh: snap: 8 (over z, x), bin: 4 (over y, core).
Axes of the slice: x: 2, y: 2, z: 4, core: 2. Of those that a mesh axis runs over, the one named last changes fastest.
Arguments:
- data: bfloat16 [256, 128, 1024], P(None, ('snap', 'bin')), may hold values from -6 to 6
- steering: bfloat16 [256, 1024, 2048], P(('snap', 'bin')), may hold values from -2 to 2
- start: float32 [256, 1024, 64], P(('snap', 'bin')), may hold values from -6 to 6
Outputs:
- projector: float32 [256, 1024, 1024], P(('snap', 'bin'))
- spectrum: float32 [2048], replicated
The draws below stay inside these ranges and needn't reach their ends.
All inputs are finite; a program needn't handle non-finite values.
Results may differ from the reference program's by a relative error of at most 0.00042.
Values may be sent and summed in bfloat16 or wider, within the bound.
A program may use at most 128 MiB of HBM per device.

```python
import math
import jax
import jax.numpy as jnp
from jax import lax

M = 1024
F = 256
SOURCES = 64
G = 2048
ITERS = 3
K2 = 128


def array_pieces(key):
    sines = jax.random.uniform(jax.random.fold_in(key, 101), (G,), jnp.float32, -1.0, 1.0)
    fraction = jax.random.uniform(jax.random.fold_in(key, 102), (F,), jnp.float32, 0.5, 1.0)
    gains = jnp.exp(jax.random.uniform(jax.random.fold_in(key, 103), (F, M), jnp.float32, -0.34, 0.34))
    return (sines, fraction, gains)


def steer_columns(fraction, gains, sines):
    half = M // 2
    places = jnp.arange(half, dtype=jnp.float32) - (half - 1) / 2.0
    phase = jnp.pi * fraction * places[:, None] * sines[None, :]
    table = jnp.concatenate([jnp.cos(phase), jnp.sin(phase)], axis=0) * 1.4142135
    return table * gains[:, None]


def draw_steering(key, part):
    sines, fraction, gains = array_pieces(key)

    def one_table(items):
        return steer_columns(items[0], items[1], sines).astype(jnp.bfloat16)
    return lax.map(one_table, (fraction, gains))


def draw_data(key, part):
    sines, fraction, gains = array_pieces(key)
    chosen = jax.random.permutation(jax.random.fold_in(key, 104), G)[:SOURCES]
    picked = jnp.take(sines, chosen)
    bulk_edge = (1.0 + (M / K2) ** 0.5) ** 2
    ratio = jnp.exp(jax.random.uniform(jax.random.fold_in(key, 105), (F, SOURCES), jnp.float32, math.log(2.5), math.log(10.0)))
    levels = jnp.sqrt(bulk_edge * ratio / M)
    bin_keys = jax.random.split(jax.random.fold_in(key, 106), F)

    def one_bin(items):
        frac, gain, level, sub_key = items
        columns = steer_columns(frac, gain, picked)
        amp_key = jax.random.fold_in(sub_key, 1)
        noise_key = jax.random.fold_in(sub_key, 2)
        amps = jax.random.truncated_normal(amp_key, -4.0, 4.0, (K2, SOURCES), jnp.float32)
        noise = jax.random.truncated_normal(noise_key, -4.0, 4.0, (K2, M), jnp.float32)
        signal = jnp.dot(amps * level[None, :], columns.T, precision=lax.Precision.HIGHEST)
        return jnp.clip(signal + noise, -6.0, 6.0).astype(jnp.bfloat16)
    return lax.map(one_bin, (fraction, gains, levels, bin_keys))


def shard_levels(key, shape, cuts, least, high):
    def one(axis_at, blocks):
        steps = jax.random.uniform(jax.random.fold_in(jax.random.fold_in(key, 6), axis_at), (blocks,), jnp.float32, least / len(cuts), high / len(cuts))
        return jnp.repeat(jnp.exp(steps), shape[axis_at] // blocks).reshape((-1,) + (1,) * (len(shape) - axis_at - 1))

    factor_of = one(*cuts[0])
    for cut in cuts[1:]:
        factor_of = factor_of * one(*cut)
    return factor_of


def bell_draw(key, extent, width, reach, pieces=(), held_as=jnp.bfloat16):
    level = shard_levels(key, extent, pieces, -0.22, 0.18) if pieces else 1.0
    values = jax.random.normal(key, extent, jnp.float32) * width * level
    return jnp.minimum(jnp.maximum(values, -reach), reach).astype(held_as)


def setup_inputs(seed: int = 0) -> dict:
    seeds = jax.random.split(jax.random.key(seed), 4)
    data = draw_data(jax.random.fold_in(seeds[3], 71), 0)
    steering = draw_steering(jax.random.fold_in(seeds[3], 71), 0)
    start = bell_draw(seeds[2], (F, M, SOURCES), 1.0, 6.0, ((0, 32),), jnp.float32)
    return {"data": data, "steering": steering, "start": start}


def one_bin(snaps, steer, basis):
    covar = jnp.dot(snaps.T.astype(jnp.float32), snaps.astype(jnp.float32), preferred_element_type=jnp.float32) / snaps.shape[0]
    for step in range(ITERS):
        image = jnp.dot(covar, basis, precision=lax.Precision.HIGHEST)
        gram_mat = jnp.dot(image.T, image, precision=lax.Precision.HIGHEST)
        lower_factor = jnp.linalg.cholesky(gram_mat)
        basis = jax.scipy.linalg.solve_triangular(lower_factor, image.T, lower=True).T
    projector = jnp.dot(basis, basis.T, precision=lax.Precision.HIGHEST)
    basis_low = basis.astype(jnp.bfloat16)
    along = jnp.dot(basis_low.T.astype(jnp.float32), steer.astype(jnp.float32), preferred_element_type=jnp.float32)
    steer_wide = steer.astype(jnp.float32)
    energy = jnp.sum(steer_wide * steer_wide, axis=0)
    noise = energy - jnp.sum(along * along, axis=0)
    return (projector, noise)

def reference(data, steering, start):
    projector, noise = lax.map(lambda items: one_bin(items[0], items[1], items[2]), (data, steering, start))
    spectrum = F * M / jnp.sum(noise, axis=0)
    return (projector, spectrum)
```

```python
import functools

import jax
import jax.numpy as jnp
from jax import lax
from jax.experimental import pallas as pl
from jax.experimental.pallas import tpu as pltpu

ITERS = 3
F32 = jnp.float32
BF16 = jnp.bfloat16
MESH = pl.DeviceIdType.MESH
VMEM_LIMIT = 64000 * 1024


def place(d, inner):
    return (d // inner, lax.rem(d, inner))


def greet_all(me, n, inner):
    barrier = pltpu.get_barrier_semaphore()

    def one(o, c):
        pl.semaphore_signal(
            barrier, inc=1, device_id=place(lax.rem(me + o, n), inner), device_id_type=MESH
        )
        return c

    lax.fori_loop(1, n, one, 0)
    pl.semaphore_wait(barrier, n - 1)


def exchange_kernel(n, inner, nb, data_ref, out_ref, send_sem, recv_sem, own_sem):
    me = lax.axis_index("snap") * inner + lax.axis_index("bin")
    own = pltpu.make_async_copy(data_ref.at[pl.ds(me * nb, nb)], out_ref.at[:, 0], own_sem)
    own.start()
    greet_all(me, n, inner)

    def copy(o):
        d = lax.rem(me + o, n)
        return pltpu.make_async_remote_copy(
            src_ref=data_ref.at[pl.ds(d * nb, nb)],
            dst_ref=out_ref.at[:, o],
            send_sem=send_sem.at[o],
            recv_sem=recv_sem.at[o],
            device_id=place(d, inner),
            device_id_type=MESH,
        )

    def start(o, c):
        copy(o).start()
        return c

    def finish(o, c):
        copy(o).wait()
        return c

    lax.fori_loop(1, n, start, 0)
    own.wait()
    lax.fori_loop(1, n, finish, 0)


def exchange(data, n, inner):
    bins, rows, width = data.shape
    nb = bins // n
    return pl.pallas_call(
        functools.partial(exchange_kernel, n, inner, nb),
        out_shape=jax.ShapeDtypeStruct((nb, n, rows, width), data.dtype),
        in_specs=[pl.BlockSpec(memory_space=pl.ANY)],
        out_specs=pl.BlockSpec(memory_space=pl.ANY),
        scratch_shapes=[
            pltpu.SemaphoreType.DMA((n,)),
            pltpu.SemaphoreType.DMA((n,)),
            pltpu.SemaphoreType.DMA,
        ],
        compiler_params=pltpu.CompilerParams(collective_id=0, has_side_effects=True),
        name="exchange",
    )(data)


def total_kernel(n, inner, scale, noise_ref, out_ref, held, send_sem, recv_sem):
    me = lax.axis_index("snap") * inner + lax.axis_index("bin")
    held[pl.ds(me, 1)] = noise_ref[...]
    greet_all(me, n, inner)

    def copy(o, slot):
        return pltpu.make_async_remote_copy(
            src_ref=noise_ref.at[0],
            dst_ref=held.at[slot],
            send_sem=send_sem.at[o],
            recv_sem=recv_sem.at[o],
            device_id=place(lax.rem(me + o, n), inner),
            device_id_type=MESH,
        )

    def start(o, c):
        copy(o, me).start()
        return c

    def finish(o, c):
        copy(o, lax.rem(me - o + n, n)).wait()
        return c

    lax.fori_loop(1, n, start, 0)
    lax.fori_loop(1, n, finish, 0)
    out_ref[...] = scale / jnp.sum(held[...], axis=0)


def total(noise, n, inner, scale):
    rows, width = noise.shape[1:]
    return pl.pallas_call(
        functools.partial(total_kernel, n, inner, scale),
        out_shape=jax.ShapeDtypeStruct((rows, width), F32),
        in_specs=[pl.BlockSpec(memory_space=pltpu.VMEM)],
        out_specs=pl.BlockSpec(memory_space=pltpu.VMEM),
        scratch_shapes=[
            pltpu.VMEM((n, rows, width), F32),
            pltpu.SemaphoreType.DMA((n,)),
            pltpu.SemaphoreType.DMA((n,)),
        ],
        compiler_params=pltpu.CompilerParams(collective_id=1, has_side_effects=True),
        name="total",
    )(noise)


def split(a):
    high = a.astype(BF16).astype(F32)
    rest = a - high
    mid = rest.astype(BF16).astype(F32)
    return high, mid, rest - mid


def stack(parts, axis):
    return jnp.concatenate(parts, axis=axis).astype(BF16)


def dot(a, b, ca, cb):
    return lax.dot_general(a, b, (((ca,), (cb,)), ((), ())), preferred_element_type=F32)


def fold_rows(p):
    r = p.shape[0] // 3
    return p[:r] + (p[r : 2 * r] + p[2 * r :])


def fold_lanes(p):
    c = p.shape[1] // 3
    return p[:, :c] + (p[:, c : 2 * c] + p[:, 2 * c :])


def inverse_factors(grams):
    size = grams[0].shape[0]
    eye = (
        lax.broadcasted_iota(jnp.int32, (size, size), 0)
        == lax.broadcasted_iota(jnp.int32, (size, size), 1)
    ).astype(F32)
    rest = [jnp.concatenate([g, eye], axis=1) for g in grams]
    wide = 2 * size
    sub = lax.broadcasted_iota(jnp.int32, (8, wide), 0)
    lane = lax.broadcasted_iota(jnp.int32, (8, size), 1)
    done = [[] for _ in grams]
    for t in range(size // 8):
        tiles = [a[8 * t : 8 * t + 8] for a in rest]
        cols = [
            [jnp.broadcast_to(a[:, 8 * t + j : 8 * t + j + 1], (8, wide)) for j in range(8)]
            for a in tiles
        ]
        invs = [jnp.zeros((8, wide), F32) for _ in tiles]
        for j in range(8):
            for i in range(len(tiles)):
                c = cols[i]
                inv = 1.0 / c[j][j : j + 1]
                below = jnp.where(sub > j, c[j], 0.0)
                tiles[i] = tiles[i] - below * (tiles[i][j : j + 1] * inv)
                for k in range(j + 1, 8):
                    c[k] = c[k] - below * (c[k][j : j + 1] * inv)
                invs[i] = jnp.where(sub == j, inv, invs[i])
        for i in range(len(tiles)):
            done[i].append(tiles[i] * jnp.sqrt(invs[i]))
            if 8 * t + 8 < size:
                scaled = (tiles[i] * invs[i])[:, :size]
                h, m, l = split(jnp.where(lane >= 8 * t + 8, scaled, 0.0))
                rh, rm, rl = split(tiles[i])
                rest[i] = rest[i] - dot(
                    stack([l, h, m, m, h, h], 0), stack([rh, rl, rm, rh, rm, rh], 0), 0, 0
                )
    return [jnp.concatenate(d, axis=0)[:, size:] for d in done]


def music_kernel(
    x_ref, start_ref, steer_ref, proj_ref, noise_ref, steer_v, out_v, s_v, v_v, in_sem, out_sem
):
    nb, kk, m = x_ref.shape
    width = start_ref.shape[2]
    g = steer_ref.shape[2]

    def load(b):
        return pltpu.make_async_copy(steer_ref.at[b], steer_v.at[b], in_sem.at[b])

    def put(b, slot):
        return pltpu.make_async_copy(out_v.at[slot], proj_ref.at[b], out_sem.at[slot])

    for b in range(nb):
        load(b).start()

    def prepare(b, c):
        x = x_ref[b]
        s_v[b] = stack(split(dot(x, x, 1, 1)), 1)
        y = dot(x, stack(split(start_ref[b]), 1), 1, 0)
        v_v[b] = fold_lanes(y).T
        return c

    lax.fori_loop(0, nb, prepare, 0)

    def step(it, c):
        last = it == ITERS - 1
        kept, grams = [], []
        for b in range(nb):
            v = v_v[b]
            vs = stack(split(v), 0)
            w = fold_rows(fold_lanes(dot(vs, s_v[b], 1, 0)))
            grams.append(fold_lanes(fold_rows(dot(stack(split(w), 0), vs, 1, 1))))
            kept.append(jnp.where(last, v, w * (1.0 / kk)))
        for b, factor in enumerate(inverse_factors(grams)):
            p = dot(stack(split(factor), 0), stack(split(kept[b]), 1), 1, 0)
            v_v[b] = fold_rows(fold_lanes(p))
        return c

    lax.fori_loop(0, ITERS, step, 0)
    noise_ref[...] = jnp.zeros_like(noise_ref)

    def finish(b, c):
        slot = lax.rem(b, 2)
        basis = fold_rows(dot(stack(split(v_v[b]), 0), x_ref[b], 1, 0))
        low = basis.astype(BF16)
        wide = low.astype(F32)
        tail = basis - wide
        left = stack([wide, tail, wide], 0)
        right = stack([wide, wide, tail], 0)

        @pl.when(b >= 2)
        def _():
            put(b - 2, slot).wait()

        step_rows = m // 4
        for r in range(0, m, step_rows):
            out_v[slot, r : r + step_rows] = dot(left[:, r : r + step_rows], right, 0, 0)
        put(b, slot).start()
        load(b).wait()
        step_lanes = g // 4
        for q in range(0, g, step_lanes):
            along = dot(low, steer_v[b, :, q : q + step_lanes], 1, 0)
            energy = jnp.zeros((8, step_lanes), F32)
            for r in range(0, m, 64):
                part = steer_v[b, r : r + 64, q : q + step_lanes].astype(F32)
                energy = energy + jnp.sum((part * part).reshape(8, 8, step_lanes), axis=0)
            noise_ref[0, :, q : q + step_lanes] += jnp.sum(energy, axis=0, keepdims=True) - jnp.sum(
                along * along, axis=0, keepdims=True
            )
        return c

    lax.fori_loop(0, nb, finish, 0)
    for b in range(max(nb - 2, 0), nb):
        put(b, b % 2).wait()


def music(x, start, steering):
    nb, kk, m = x.shape
    width = start.shape[2]
    g = steering.shape[2]
    return pl.pallas_call(
        music_kernel,
        out_shape=(
            jax.ShapeDtypeStruct((nb, m, m), F32),
            jax.ShapeDtypeStruct((1, 1, g), F32),
        ),
        in_specs=[
            pl.BlockSpec(memory_space=pltpu.VMEM),
            pl.BlockSpec(memory_space=pltpu.VMEM),
            pl.BlockSpec(memory_space=pl.ANY),
        ],
        out_specs=(
            pl.BlockSpec(memory_space=pl.ANY),
            pl.BlockSpec(memory_space=pltpu.VMEM),
        ),
        scratch_shapes=[
            pltpu.VMEM((nb, m, g), BF16),
            pltpu.VMEM((2, m, m), F32),
            pltpu.VMEM((nb, kk, 3 * kk), BF16),
            pltpu.VMEM((nb, width, kk), F32),
            pltpu.SemaphoreType.DMA((nb,)),
            pltpu.SemaphoreType.DMA((2,)),
        ],
        compiler_params=pltpu.CompilerParams(vmem_limit_bytes=VMEM_LIMIT),
        name="music",
    )(x, start, steering)


def on_device(n, inner, data, steering, start):
    bins, rows, m = data.shape
    owned = exchange(data, n, inner)
    owned = owned.reshape(owned.shape[0], n * rows, m)
    projector, noise = music(owned, start, steering)
    spectrum = total(noise, n, inner, float(bins * m))
    return (projector, spectrum.reshape(-1))


def solution(mesh):
    P = jax.sharding.PartitionSpec
    inner = mesh.shape["bin"]
    n = mesh.shape["snap"] * inner
    both = ("snap", "bin")
    return jax.shard_map(
        functools.partial(on_device, n, inner),
        mesh=mesh,
        in_specs=(P(None, both, None), P(both, None, None), P(both, None, None)),
        out_specs=(P(both, None, None), P()),
        check_vma=False,
    )
```
